32 devices in a mesh: node: 8 (over z, x), local: 4 (over y, core).
Axes of the slice: x: 2, y: 2, z: 4, core: 2. Of those that a mesh axis runs over, the one named last changes fastest.
Arguments:
- gate_pre: bfloat16 [3584, 15360], P('node', 'local'), may hold values from -6 to 6
- up_pre: bfloat16 [3584, 15360], P('node', 'local'), may hold values from -6 to 6
- out_grad: bfloat16 [3584, 4096], P('node', 'local'), may hold values from -6 to 6
Outputs:
- weight_grad: float32 [15360, 4096], P('local', 'node')
The draws below stay inside these ranges and needn't reach their ends.
All inputs are finite; a program needn't handle non-finite values.
Results may differ from the reference program's by a relative error of at most 0.015.
Values may be sent and summed in bfloat16 or wider, within the bound.
No kernel may reach another device: no remote copies, remote signals or barrier semaphores. Data moves between devices by JAX's collectives and lax.ppermute only.
A program may use at most 128 MiB of HBM per device.

```python
import jax
import jax.numpy as jnp
from jax import lax

D = 4096
BUCKET = 15360
TOK_DEV = 448
TOKENS = 3584
N_NODE = 8


def strengthened(result, own_key, source, target, parts, factor):
    def block_of(axis_at):
        return (jnp.arange(result.shape[axis_at]) // (result.shape[axis_at] // parts)).reshape((-1,) + (1,) * (result.ndim - 1 - axis_at))

    near = jax.random.permutation(own_key, parts)[block_of(target)]
    other_side = (block_of(target) + parts // 2) % parts
    return jnp.where((block_of(source) == near) | (block_of(source) == other_side), factor * result, result)


def shard_levels(rng, extent, cuts, low, largest):
    def one(axis_at, parts):
        steps = jax.random.uniform(jax.random.fold_in(jax.random.fold_in(rng, 6), axis_at), (parts,), jnp.float32, low / len(cuts), largest / len(cuts))
        return jnp.repeat(jnp.exp(steps), extent[axis_at] // parts).reshape((-1,) + (1,) * (len(extent) - axis_at - 1))

    factor_of = one(*cuts[0])
    for cut in cuts[1:]:
        factor_of = factor_of * one(*cut)
    return factor_of


def centred(rng, shape, spread, most, pieces=(), held_as=jnp.bfloat16):
    values = spread * jax.random.normal(rng, shape, jnp.float32)
    if pieces:
        values = values * shard_levels(rng, shape, pieces, -0.22, 0.18)
    return jnp.clip(values, -most, most).astype(held_as)


def noise_with(key, shape, width, reach, cuts, heavy, dtype=jnp.bfloat16):
    result = width * jax.random.normal(key, shape, jnp.float32)
    if cuts:
        result = result * shard_levels(key, shape, cuts, -0.22, 0.18)
    return jnp.clip(strengthened(result, jax.random.fold_in(key, 3), *heavy), -reach, reach).astype(dtype)


def setup_inputs(seed: int = 0) -> dict:
    key_of = jax.random.split(jax.random.key(seed), 4)
    gate_pre = centred(key_of[0], (TOKENS, BUCKET), 1.0, 6.0, ((0, 8), (1, 4)))
    up_pre = centred(key_of[1], (TOKENS, BUCKET), 1.0, 6.0, ((0, 8), (1, 4)))
    out_grad = noise_with(key_of[2], (TOKENS, D), 1.0, 6.0, ((0, 8), (1, 4)), (0, 1, 8, 2.0))
    return {"gate_pre": gate_pre, "up_pre": up_pre, "out_grad": out_grad}


def reference(gate_pre, up_pre, out_grad):
    averaging = 1.0 / N_NODE

    def advance(accumulated, inputs):
        gate_block, up_block, grad_block = inputs
        gate_float = gate_block.astype(jnp.float32)
        activated = gate_float * jax.nn.sigmoid(gate_float)
        hidden = (activated * up_block.astype(jnp.float32)).astype(jnp.bfloat16)
        product = lax.dot_general(hidden.astype(jnp.float32), grad_block.astype(jnp.float32), (((0,), (0,)), ((), ())), preferred_element_type=jnp.float32)
        term = (product * averaging).astype(jnp.bfloat16)
        return accumulated + term.astype(jnp.float32), None

    initial = jnp.zeros((BUCKET, D), jnp.float32)
    stacked = (gate_pre.reshape(N_NODE, TOK_DEV, BUCKET), up_pre.reshape(N_NODE, TOK_DEV, BUCKET), out_grad.reshape(N_NODE, TOK_DEV, D))
    total, unused = lax.scan(advance, initial, stacked)
    return total
```

```python
import math

import jax
import jax.numpy as jnp
from jax import lax
from jax.sharding import PartitionSpec as P


PLAN = ((5, "B"), (5, "A"), (5, "B"), (5, "A"), (4, "B"), (3, "A"), (2, "A"), (1, "A"))


def cuts(rows, plan):
    unit = math.gcd(rows, 128)
    tiles, whole = rows // unit, sum(share for share, _ in plan)
    edges, done = [0], 0
    for share, _ in plan:
        done += share
        edges.append(round(tiles * done / whole) * unit)
    return [(a, b - a, kind) for a, b, (_, kind) in zip(edges, edges[1:], plan) if b > a]


def contract(left, right, dtype=jnp.float32):
    out = lax.dot_general(left, right, (((0,), (0,)), ((), ())), preferred_element_type=jnp.float32)
    return out.astype(dtype)


def solution(mesh):
    nodes, locals_ = mesh.shape["node"], mesh.shape["local"]
    n_x = max(d for d in range(1, math.isqrt(nodes) + 1) if nodes % d == 0 and nodes // d % 2 == 0)
    n_z = nodes // n_x
    half = n_z // 2
    masks = [locals_ >> (i + 1) for i in range(locals_.bit_length() - 1)]

    def z_of(side, r):
        return half - 1 - r if side == 0 else half + r

    def along(moves):
        return [
            (z_of(s, a) * n_x + x, z_of(t, b) * n_x + x)
            for s, a, t, b in moves
            for x in range(n_x)
        ]

    inward = [along([(s, r + 1, s, r) for s in (0, 1) for r in range(half - k)]) for k in range(1, half)]
    across = along([(0, 0, 1, 0), (1, 0, 0, 0)])
    outward = [along([(s, k - 1, s, k) for s in (0, 1)]) for k in range(1, half)]
    turn = [
        [(z * n_x + x, z * n_x + (x + j) % n_x) for z in range(n_z) for x in range(n_x)]
        for j in range(n_x)
    ]

    def body(gate, up, grad):
        node, lane = lax.axis_index("node"), lax.axis_index("local")
        z, x = node // n_x, node % n_x
        side = z // half
        r = jnp.where(side == 0, half - 1 - z, z - half)
        tokens, rows = gate.shape
        width = grad.shape[1] * locals_ // nodes
        per_piece = nodes // locals_
        quarter = tokens // locals_

        def gathered(piece):
            arr = piece.reshape((1,) * len(masks) + piece.shape)
            for i, mask in enumerate(masks):
                other = lax.ppermute(arr, "local", [(l, l ^ mask) for l in range(locals_)])
                arr = jnp.where(
                    (lane & mask) != 0,
                    jnp.concatenate([other, arr], axis=i),
                    jnp.concatenate([arr, other], axis=i),
                )
            return arr.reshape((locals_,) + piece.shape)

        pieces = gathered(grad)

        def block(side_, r_, j, first, count):
            z_ = jnp.where(side_ == 0, half - 1 - r_, half + r_)
            b = z_ * n_x + (x + j) % n_x
            at = (b // per_piece, first, (b % per_piece) * width)
            return lax.dynamic_slice(pieces, at, (1, count, width))[0]

        def share_of(side_, r_):
            return [block(side_, r_, j, lane * quarter, quarter) for j in range(n_x)]

        def cat(parts, axis=1):
            return parts[0] if len(parts) == 1 else jnp.concatenate(parts, axis=axis)

        block_w = n_x * width
        to_other = cat(sum([share_of(1 - side, q) for q in range(half)], []))
        to_side = cat(sum([share_of(side, q) for q in range(half - 1)], []) + [to_other]) if half > 1 else None

        def whole_rows(piece):
            return gathered(piece).reshape(tokens, piece.shape[1])

        crossed = [whole_rows(lax.ppermute(to_other, "node", across))]
        nearer = []
        passed = to_side
        for k in range(1, half):
            passed = lax.ppermute(passed, "node", inward[k - 1])
            over = lax.ppermute(passed[:, (half - 1) * block_w:], "node", across)
            own = lax.dynamic_slice(passed, (0, jnp.minimum(r, half - 2) * block_w), (quarter, block_w)) if half > 2 else passed[:, :block_w]
            both = whole_rows(cat([own, over]))
            nearer.append(both[:, :block_w])
            crossed.append(both[:, block_w:])

        def factor(j):
            mine = cat([block(side, jnp.minimum(r + q, half - 1), j, 0, tokens) for q in range(half)])
            parts = [mine]
            for g in nearer:
                rest = jnp.zeros((tokens, (half - 1) * width), g.dtype)
                parts.append(cat([g[:, j * width:(j + 1) * width], rest]))
            for g in crossed:
                parts.append(cat([g[:, q * block_w + j * width:q * block_w + (j + 1) * width] for q in range(half)]))
            return cat(parts, axis=0)

        factors = [factor(j) for j in range(n_x)]

        out = jnp.zeros((rows, width), jnp.float32)
        for start, count, kind in cuts(rows, PLAN):
            g = gate[:, start:start + count].astype(jnp.float32)
            u = up[:, start:start + count].astype(jnp.float32)
            hidden = (g * jax.nn.sigmoid(g) * u).astype(jnp.bfloat16)
            near, passed = [], hidden
            over = [lax.ppermute(hidden, "node", across)]
            for k in range(1, half):
                passed = lax.ppermute(passed, "node", inward[k - 1])
                near.append(passed)
                over.append(lax.ppermute(passed, "node", across))
            left = cat([hidden] + near + over, axis=0)
            sends = [contract(left, factors[j], jnp.bfloat16) for j in range(1, n_x)]
            keep = contract(left, factors[0])
            if kind == "A":
                for j in range(1, n_x):
                    keep = keep + lax.ppermute(sends[j - 1], "node", turn[j]).astype(jnp.float32)
                total, away = keep[:, :width], keep[:, width:]
                for k in range(1, half):
                    came = lax.ppermute(away[:, :(half - k) * width].astype(jnp.bfloat16), "node", outward[k - 1]).astype(jnp.float32)
                    total = total + came[:, :width]
                    if k < half - 1:
                        away = away[:, :(half - k - 1) * width] + came[:, width:]
            else:
                groups = [keep] + sends
                own = [s[:, :width].astype(jnp.float32) for s in groups]
                away = [s[:, width:].astype(jnp.float32) for s in groups]
                for k in range(1, half):
                    w = (half - k) * width
                    came = lax.ppermute(cat([a[:, :w].astype(jnp.bfloat16) for a in away]), "node", outward[k - 1]).astype(jnp.float32)
                    came = [came[:, j * w:(j + 1) * w] for j in range(n_x)]
                    own = [o + c[:, :width] for o, c in zip(own, came)]
                    if k < half - 1:
                        away = [a[:, :w - width] + c[:, width:] for a, c in zip(away, came)]
                total = own[0]
                for j in range(1, n_x):
                    total = total + lax.ppermute(own[j].astype(jnp.bfloat16), "node", turn[j]).astype(jnp.float32)
            out = lax.dynamic_update_slice(out, total, (start, 0))
        return out * (1.0 / nodes)

    placed = (P("node", "local"), P("node", "local"), P("node", "local"))
    return jax.shard_map(body, mesh=mesh, in_specs=placed, out_specs=P("local", "node"), check_vma=False)
```
